256 devices in a mesh: dp: 128 (over z, y_lo, x, core), mp: 2 (over y_hi).
Axes of the slice: x: 4, y: 4 (y_hi: 2, y_lo: 2; y = y_hi * 2 + y_lo), z: 8, core: 2. Of those that a mesh axis runs over, the one named last changes fastest.
Arguments:
- context: bfloat16 [40960, 2048], P('dp', 'mp'), may hold values from -24 to 24
- out_weight: bfloat16 [2048, 3584], P('mp'), may hold values from -0.125 to 0.125
- cotangent: bfloat16 [40960, 3584], P('dp'), may hold values from -0.059814453 to 0.059814453
- norm_gain: float32 [3584], replicated, may hold values from 0.5 to 1.5
- first_moment: float32 [2, 1024, 3584], P('mp', 'dp'), may hold values from -6 to 6
- second_moment: float32 [2, 1024, 3584], P('mp', 'dp'), may hold values from 0.01 to 1
Outputs:
- new_weight: bfloat16 [2, 1024, 3584], P('mp', 'dp')
- new_first: float32 [2, 1024, 3584], P('mp', 'dp')
- new_second: float32 [2, 1024, 3584], P('mp', 'dp')
- grad_gain: float32 [3584], replicated
- grad_context: bfloat16 [40960, 2048], P('dp', 'mp')
The draws below stay inside these ranges and needn't reach their ends.
All inputs are finite; a program needn't handle non-finite values.
Results may differ from the reference program's by a relative error of at most 0.005.
Values may be sent and summed in bfloat16 or wider, within the bound.
No kernel may reach another device: no remote copies, remote signals or barrier semaphores. Data moves between devices by JAX's collectives and lax.ppermute only.
A program may use at most 128 MiB of HBM per device.

```python
import math
import jax
import jax.numpy as jnp
from jax import lax

D = 3584
HQ = 2048
TOKENS = 40960
N_MP = 2


def with_spikes(result, own_key, source, target, parts, factor):
    def block_of(position):
        return (jnp.arange(result.shape[position]) // (result.shape[position] // parts)).reshape((-1,) + (1,) * (result.ndim - 1 - position))

    one_side = jax.random.permutation(own_key, parts)[block_of(target)]
    second = (block_of(target) + parts // 2) % parts
    return jnp.where((block_of(source) == one_side) | (block_of(source) == second), factor * result, result)


def shard_levels(stream_key, extent, split, least, high):
    gain, own = 1.0, jax.random.fold_in(stream_key, 6)
    for position, blocks in split:
        steps = jnp.exp(jax.random.uniform(jax.random.fold_in(own, position), (blocks,), jnp.float32, least / len(split), high / len(split)))
        gain = gain * jnp.repeat(steps, extent[position] // blocks).reshape([-1 if axis == position else 1 for axis in range(len(extent))])
    return gain


def centred(key, extent, spread, reach, pieces=(), dtype=jnp.bfloat16):
    gain = shard_levels(key, extent, pieces, -0.22, 0.18) if pieces else 1.0
    entries = jax.random.normal(key, extent, jnp.float32) * spread * gain
    return jnp.minimum(jnp.maximum(entries, -reach), reach).astype(dtype)


def gaussian_with(own_key, shape, width, limit, cuts, heavy, held_as=jnp.bfloat16):
    array = width * jax.random.normal(own_key, shape, jnp.float32)
    if cuts:
        array = array * shard_levels(own_key, shape, cuts, -0.22, 0.18)
    return jnp.clip(with_spikes(array, jax.random.fold_in(own_key, 3), *heavy), -limit, limit).astype(held_as)


def setup_inputs(seed: int = 0) -> dict:
    arg_keys = jax.random.split(jax.random.key(seed), 7)
    return {
        "context": gaussian_with(arg_keys[0], (TOKENS, HQ), 1.0, 24.0, ((0, 128), (1, 2)), (0, 1, 128, 5.5)),
        "out_weight": centred(arg_keys[1], (HQ, D), HQ ** -0.5, 0.125, ((0, 2),)),
        "cotangent": centred(arg_keys[2], (TOKENS, D), 0.01, 0.059814453, ((0, 128),)),
        "norm_gain": jnp.clip(1.0 + 0.1 * jax.random.normal(arg_keys[3], (D,), jnp.float32), 0.5, 1.5),
        "first_moment": centred(arg_keys[4], (N_MP, HQ // N_MP, D), 1.0, 6.0, ((0, 2), (1, 128)), jnp.float32),
        "second_moment": jnp.clip(jnp.exp(math.log(1.0) - 4.6051702 * jax.random.uniform(arg_keys[5], (N_MP, HQ // N_MP, D), jnp.float32) ** shard_levels(arg_keys[5], (N_MP, HQ // N_MP, D), ((0, 2), (1, 128)), -0.2, 0.2)), 0.01, 1.0),
    }


norm_floor = 0.1
learn_rate = 0.01
beta_one = 0.9
beta_two = 0.95
adam_floor = 1e-08

def reference(context, out_weight, cotangent, norm_gain, first_moment, second_moment):
    attn = jnp.dot(context, out_weight, preferred_element_type=jnp.float32)
    inverse = lax.rsqrt(lax.optimization_barrier(jnp.mean(attn * attn, axis=-1, keepdims=True)) + norm_floor)
    normed = attn * inverse
    upstream = cotangent.astype(jnp.float32)
    scaled = upstream * norm_gain
    grad_gain = lax.optimization_barrier(jnp.sum(upstream * normed, axis=0))
    grad_attn = (inverse * (scaled - normed * lax.optimization_barrier(jnp.mean(scaled * normed, axis=-1, keepdims=True)))).astype(jnp.bfloat16)
    grad_context = jnp.dot(grad_attn, out_weight.T, preferred_element_type=jnp.float32).astype(jnp.bfloat16)
    grad_weight = jnp.dot(context.T, grad_attn, preferred_element_type=jnp.float32)
    grad_weight = grad_weight.reshape(N_MP, HQ // N_MP, D)
    new_first = beta_one * first_moment + (1.0 - beta_one) * grad_weight
    new_second = beta_two * second_moment + (1.0 - beta_two) * grad_weight * grad_weight
    master = out_weight.astype(jnp.float32).reshape(N_MP, HQ // N_MP, D)
    new_weight = (master - learn_rate * new_first / (jnp.sqrt(new_second) + adam_floor)).astype(jnp.bfloat16)
    return (new_weight, new_first, new_second, grad_gain, grad_context)
```

```python
import jax
import jax.numpy as jnp
from jax import lax
from jax.sharding import Mesh
from jax.sharding import PartitionSpec as P

DP = ("dp_0", "dp_1", "dp_2", "dp_3")
Z, YL, X, C, MP = "dp_0", "dp_1", "dp_2", "dp_3", "mp"

norm_floor = 0.1
learn_rate = 0.01
beta_one = 0.9
beta_two = 0.95
adam_floor = 1e-08

CHUNKS = 2
BF = jnp.bfloat16
F32 = jnp.float32
SWAP = [(0, 1), (1, 0)]
PAIR_A = [(i, i ^ 1) for i in range(4)]
PAIR_B = [(i, 3 - i) for i in range(4)]


def dot(a, b):
    return jnp.dot(a, b, preferred_element_type=F32)


def picked(array, index):
    return lax.dynamic_index_in_dim(array, index, 0, keepdims=False)


def transposed_context(context, mp):
    half = context.shape[0] // 2
    core, x = lax.axis_index(C), lax.axis_index(X)
    halves = context.reshape(2, half, -1)
    ordered = jnp.concatenate([picked(halves, mp), picked(halves, 1 - mp)], 0)
    rows = ordered.T.reshape(16, 4, 2, 8, 2 * half).transpose(2, 1, 0, 3, 4)
    other = lax.ppermute(picked(rows, 1 - core), C, SWAP)
    rows = jnp.concatenate([picked(rows, core), other], -1)
    near, far, across = x ^ 1, 3 - x, (x + 2) % 4
    first, last = rows[:, :8], rows[:, 8:]
    order = [
        picked(first, near),
        picked(first, across),
        picked(last, far),
        picked(last, across),
        picked(first, x),
        picked(first, far),
        picked(last, x),
        picked(last, near),
    ]
    return jnp.concatenate(order, 0).reshape(512, -1)


def reduced(context_rows, grads):
    width = grads.shape[1]
    sent = dot(context_rows[:256], grads).astype(BF)
    got_a = lax.ppermute(sent[:128], X, PAIR_A)
    got_b = lax.ppermute(sent[128:], X, PAIR_B)
    kept = dot(context_rows[256:], grads)
    sum_a = kept[:128] + got_a.astype(F32)
    sum_b = kept[128:] + got_b.astype(F32)
    more_a = lax.ppermute(sum_a[64:].astype(BF), X, PAIR_B)
    more_b = lax.ppermute(sum_b[64:].astype(BF), X, PAIR_A)
    tile_a = sum_a[:64] + more_a.astype(F32)
    tile_b = sum_b[:64] + more_b.astype(F32)
    tiles = jnp.concatenate([tile_a.astype(BF), tile_b.astype(BF)], 0).reshape(16, 8, width)
    tiles = lax.all_to_all(tiles, (Z, YL), split_axis=0, concat_axis=0, tiled=True)
    return tiles.astype(F32).sum(0)


def summed_everywhere(part):
    part = part + lax.ppermute(part, C, SWAP)
    part = part + lax.ppermute(part, MP, SWAP)
    part = part + lax.ppermute(part, X, PAIR_A)
    part = part + lax.ppermute(part, X, PAIR_B)
    copies = jnp.broadcast_to(part, (16, *part.shape))
    return lax.all_to_all(copies, (Z, YL), split_axis=0, concat_axis=0, tiled=True).sum(0)


def adam_update(master, first_moment, second_moment, grad_shard):
    new_first = beta_one * first_moment + (1.0 - beta_one) * grad_shard
    new_second = beta_two * second_moment + (1.0 - beta_two) * grad_shard * grad_shard
    new_weight = (master - learn_rate * new_first / (jnp.sqrt(new_second) + adam_floor)).astype(BF)
    return (new_weight, new_first, new_second)


def per_device(context, out_weight, cotangent, norm_gain, first_moment, second_moment):
    tokens, width = cotangent.shape
    half = tokens // 2
    mp = lax.axis_index(MP)
    mine = lax.dynamic_slice_in_dim(context, mp * half, half, 0)
    theirs = lax.dynamic_slice_in_dim(context, (1 - mp) * half, half, 0)
    sent = dot(theirs, out_weight).astype(BF)
    got = lax.ppermute(sent, MP, SWAP)
    own = dot(mine, out_weight)
    context_rows = transposed_context(context, mp)
    upstream = lax.dynamic_slice_in_dim(cotangent, mp * half, half, 0).astype(F32)

    attn = own + got.astype(F32)
    inverse = lax.rsqrt(jnp.mean(attn * attn, axis=-1, keepdims=True) + norm_floor)
    normed = attn * inverse
    scaled = upstream * norm_gain
    product = jnp.mean(scaled * normed, axis=-1, keepdims=True)
    grad_attn = (inverse * (scaled - normed * product)).astype(BF)
    grad_gain = summed_everywhere(jnp.sum(upstream * normed, axis=0))

    step = width // CHUNKS
    near = lax.ppermute(grad_attn, C, SWAP)
    arrived, shards = [], []
    for k in range(CHUNKS):
        cols = slice(k * step, (k + 1) * step)
        other = lax.ppermute(grad_attn[:, cols], MP, SWAP)
        other_near = lax.ppermute(other, C, SWAP)
        grads = jnp.concatenate([grad_attn[:, cols], other, near[:, cols], other_near], 0)
        shards.append(reduced(context_rows, grads))
        arrived.append(other)
    grad_shard = jnp.concatenate(shards, 1)

    def back(grads):
        return lax.dot_general(
            grads, out_weight, (((1,), (1,)), ((), ())), preferred_element_type=F32
        ).astype(BF)

    back_mine = back(grad_attn)
    back_theirs = back(jnp.concatenate(arrived, 1))
    pair = jnp.stack([back_mine, back_theirs])
    grad_context = jnp.concatenate([picked(pair, mp), picked(pair, 1 - mp)], 0)

    shard_rows = first_moment.shape[1]
    master = lax.dynamic_slice_in_dim(
        out_weight, lax.axis_index(DP) * shard_rows, shard_rows, 0
    ).astype(F32)[None]
    new_weight, new_first, new_second = adam_update(
        master, first_moment, second_moment, grad_shard[None]
    )
    return (new_weight, new_first, new_second, grad_gain, grad_context)


def solution(mesh):
    finer = Mesh(
        mesh.devices.reshape(8, 2, 4, 2, mesh.shape["mp"]), ("dp_0", "dp_1", "dp_2", "dp_3", "mp")
    )
    placed = (P(DP, "mp"), P("mp", None), P(DP, None), P(), P("mp", DP, None), P("mp", DP, None))
    return jax.shard_map(
        per_device,
        mesh=finer,
        in_specs=placed,
        out_specs=(P("mp", DP, None), P("mp", DP, None), P("mp", DP, None), P(), P(DP, "mp")),
        check_vma=False,
    )
```

```python
import jax
import jax.numpy as jnp
from jax import lax
from jax.sharding import Mesh
from jax.sharding import PartitionSpec as P


DP = ("dp_0", "dp_1", "dp_2", "dp_3")
Z, YL, X, C, MP = "dp_0", "dp_1", "dp_2", "dp_3", "mp"

norm_floor = 0.1
learn_rate = 0.01
beta_one = 0.9
beta_two = 0.95
adam_floor = 1e-08

FORWARD = (1024, 2560)
WIDTHS = (896, 1280, 1408)
BF = jnp.bfloat16
F32 = jnp.float32
SWAP = [(0, 1), (1, 0)]
SHIFTS = [[(i, (i + j) % 4) for i in range(4)] for j in range(4)]


def dot(a, b):
    return jnp.dot(a, b, preferred_element_type=F32)


def picked(array, index):
    return lax.dynamic_index_in_dim(array, index, 0, keepdims=False)


def after(value, *others):
    return lax.optimization_barrier((value, *others))[0]


def cut(array, widths):
    begin, pieces = 0, []
    for size in widths:
        pieces.append(array[:, begin : begin + size])
        begin += size
    return pieces


def transposed_context(context, mp):
    half = context.shape[0] // 2
    core, x = lax.axis_index(C), lax.axis_index(X)
    halves = context.reshape(2, half, -1)
    ordered = jnp.concatenate([picked(halves, mp), picked(halves, 1 - mp)], 0)
    rows = ordered.T.reshape(16, 4, 2, 8, 2 * half).transpose(2, 1, 0, 3, 4)
    other = lax.ppermute(picked(rows, 1 - core), C, SWAP)
    rows = jnp.concatenate([picked(rows, core), other], -1)
    return [picked(rows, (x + j) % 4).reshape(128, -1) for j in range(4)]


def packed(gain):
    high = lax.reduce_precision(gain, 8, 7)
    return jnp.concatenate([high, gain - high], 0).astype(BF)


def unpacked(rows):
    rows = rows.astype(F32)
    return rows[..., :4, :] + rows[..., 4:, :]


def adam_update(master, first_moment, second_moment, grad_shard):
    new_first = beta_one * first_moment + (1.0 - beta_one) * grad_shard
    new_second = beta_two * second_moment + (1.0 - beta_two) * grad_shard * grad_shard
    new_weight = (master - learn_rate * new_first / (jnp.sqrt(new_second) + adam_floor)).astype(BF)
    return (new_weight, new_first, new_second)


def per_device(context, out_weight, cotangent, norm_gain, first_moment, second_moment):
    tokens, width = cotangent.shape
    half = tokens // 2
    mp = lax.axis_index(MP)
    mine = lax.dynamic_slice_in_dim(context, mp * half, half, 0)
    theirs = lax.dynamic_slice_in_dim(context, (1 - mp) * half, half, 0)
    got = [
        lax.ppermute(dot(theirs, columns).astype(BF), MP, SWAP)
        for columns in cut(out_weight, FORWARD)
    ]
    own = dot(mine, out_weight)
    context_rows = transposed_context(context, mp)
    got, own, context_rows = lax.optimization_barrier((got, own, context_rows))
    upstream = lax.dynamic_slice_in_dim(cotangent, mp * half, half, 0).astype(F32)

    attn = own + jnp.concatenate(got, 1).astype(F32)
    inverse = lax.rsqrt(jnp.mean(attn * attn, axis=-1, keepdims=True) + norm_floor)
    normed = attn * inverse
    scaled = upstream * norm_gain
    product = jnp.mean(scaled * normed, axis=-1, keepdims=True)
    grad_attn = (inverse * (scaled - normed * product)).astype(BF)
    gain = jnp.sum(upstream * normed, axis=0).reshape(4, -1)

    mine = cut(grad_attn, WIDTHS)
    mine[0] = jnp.concatenate([mine[0], packed(gain)], 0)
    theirs = [lax.ppermute(piece, MP, SWAP) for piece in mine]
    near = [lax.ppermute(piece, C, SWAP) for piece in mine]

    kept, shifted = [], []
    for k, other in enumerate(theirs):
        other_near = lax.ppermute(other, C, SWAP)
        parts = [mine[k], other, near[k], other_near]
        grads = jnp.concatenate([part[:half] for part in parts], 0)
        sent = [dot(rows, grads).astype(BF) for rows in context_rows[1:]]
        kept.append(dot(context_rows[0], grads))
        if k == 0:
            gain += sum(unpacked(part[half:]) for part in parts[1:])
            sent = [jnp.concatenate([part, packed(gain)], 0) for part in sent]
        else:
            shifted[-1] = [after(part, kept[-1]) for part in shifted[-1]]
        shifted.append([lax.ppermute(part, X, SHIFTS[j + 1]) for j, part in enumerate(sent)])

    both = jnp.concatenate([after(part[:half], *sent) for part in (*mine, *theirs)], 1)
    both = jnp.concatenate([both[:, :width], both[:, width:]], 0)
    back = lax.dot_general(
        both, out_weight, (((1,), (1,)), ((), ())), preferred_element_type=F32
    ).astype(BF)
    *shifted[-1], back = lax.optimization_barrier((*shifted[-1], back))

    tiles = []
    for k, arrived in enumerate(shifted):
        total = (kept[k] + sum(part[:128].astype(F32) for part in arrived)).astype(BF)
        tile = total.reshape(16, 8, -1)
        if k == 0:
            gain += sum(unpacked(part[128:]) for part in arrived)
            copies = jnp.broadcast_to(packed(gain), tile.shape)
            tile = jnp.concatenate([tile, copies], 1)
        tile = lax.all_to_all(tile, (Z, YL), split_axis=0, concat_axis=0, tiled=True)
        if k == 0:
            grad_gain = unpacked(tile[:, 8:]).sum(0).reshape(-1)
        tiles.append(tile[:, :8].astype(F32).sum(0))
    grad_shard = jnp.concatenate(tiles, 1)
    pair = back.reshape(2, half, -1)
    grad_context = jnp.concatenate([picked(pair, mp), picked(pair, 1 - mp)], 0)

    shard_rows = first_moment.shape[1]
    master = lax.dynamic_slice_in_dim(
        out_weight, lax.axis_index(DP) * shard_rows, shard_rows, 0
    ).astype(F32)[None]
    new_weight, new_first, new_second = adam_update(
        master, first_moment, second_moment, grad_shard[None]
    )
    return (new_weight, new_first, new_second, grad_gain, grad_context)


def solution(mesh):
    finer = Mesh(
        mesh.devices.reshape(8, 2, 4, 2, mesh.shape["mp"]), ("dp_0", "dp_1", "dp_2", "dp_3", "mp")
    )
    placed = (P(DP, "mp"), P("mp", None), P(DP, None), P(), P("mp", DP, None), P("mp", DP, None))
    return jax.shard_map(
        per_device,
        mesh=finer,
        in_specs=placed,
        out_specs=(P("mp", DP, None), P("mp", DP, None), P("mp", DP, None), P(), P(DP, "mp")),
        check_vma=False,
    )
```

```python
import jax
import jax.numpy as jnp
from jax import lax
from jax.sharding import Mesh
from jax.sharding import PartitionSpec as P


DP = ("z_1", "z_0", "y_0", "x", "core")
QUAD, PARITY, YL, X, C = DP
Z = (QUAD, PARITY)
MP = "mp"

norm_floor = 0.1
learn_rate = 0.01
beta_one = 0.9
beta_two = 0.95
adam_floor = 1e-08

FORWARD = (1024, 2560)
WIDTHS = (2048, 1536)
BF = jnp.bfloat16
F32 = jnp.float32
SWAP = [(0, 1), (1, 0)]
NEAR = (X, [(i, i ^ 1) for i in range(4)])
FAR = (X, [(i, 3 - i) for i in range(4)])
EVEN = (Z, [(i, i ^ 1) for i in range(8)])
ODD = (Z, [(i, (i + 2 * (i % 2) - 1) % 8) for i in range(8)])
ROUTES = {"a": (NEAR, FAR, EVEN), "b": (FAR, NEAR, ODD), "c": (EVEN, NEAR, FAR), "d": (ODD, FAR, NEAR)}


def dot(a, b):
    return jnp.dot(a, b, preferred_element_type=F32)


def picked(array, index):
    return lax.dynamic_index_in_dim(array, index, 0, keepdims=False)


def after(value, *others):
    return lax.optimization_barrier((value, *others))[0]


def moved(value, axis, pairs):
    return lax.ppermute(value, axis, pairs)


def cut(array, widths):
    begin, pieces = 0, []
    for size in widths:
        pieces.append(array[:, begin : begin + size])
        begin += size
    return pieces


def transposed_context(context, mp):
    half = context.shape[0] // 2
    core, x, parity = lax.axis_index(C), lax.axis_index(X), lax.axis_index(PARITY)
    halves = context.reshape(2, half, -1)
    ordered = jnp.concatenate([picked(halves, mp), picked(halves, 1 - mp)], 0)
    rows = ordered.T.reshape(4, 2, 2, 4, 2, 8, 2 * half).transpose(4, 3, 1, 0, 2, 5, 6)
    other = moved(picked(rows, 1 - core), C, SWAP)
    rows = jnp.concatenate([picked(rows, core), other], -1).reshape(4, 2, 64, 2 * 2 * half)

    def block(owner, same):
        return picked(picked(rows, owner), parity if same else 1 - parity)

    at, near, far, across = x, x ^ 1, 3 - x, 3 - (x ^ 1)
    places = {
        "a": ([(near, 1), (near, 0), (across, 1), (across, 0)], [(at, 1), (at, 0), (far, 1), (far, 0)]),
        "b": ([(far, 1), (far, 0), (across, 1), (across, 0)], [(at, 1), (at, 0), (near, 1), (near, 0)]),
        "c": tuple([(owner, same) for owner in (at, far, near, across)] for same in (0, 1)),
        "d": tuple([(owner, same) for owner in (at, near, far, across)] for same in (0, 1)),
    }
    return {
        part: [jnp.concatenate([block(*place) for place in side], 0) for side in sides]
        for part, sides in places.items()
    }


def packed(gain):
    high = lax.reduce_precision(gain, 8, 7)
    return jnp.concatenate([high, gain - high], 0).astype(BF)


def unpacked(rows):
    rows = rows.astype(F32)
    return rows[..., :4, :] + rows[..., 4:, :]


def adam_update(master, first_moment, second_moment, grad_shard):
    new_first = beta_one * first_moment + (1.0 - beta_one) * grad_shard
    new_second = beta_two * second_moment + (1.0 - beta_two) * grad_shard * grad_shard
    new_weight = (master - learn_rate * new_first / (jnp.sqrt(new_second) + adam_floor)).astype(BF)
    return (new_weight, new_first, new_second)


def per_device(context, out_weight, cotangent, norm_gain, first_moment, second_moment):
    tokens, width = cotangent.shape
    half = tokens // 2
    mp = lax.axis_index(MP)
    mine = lax.dynamic_slice_in_dim(context, mp * half, half, 0)
    theirs = lax.dynamic_slice_in_dim(context, (1 - mp) * half, half, 0)
    got = [moved(dot(theirs, columns).astype(BF), MP, SWAP) for columns in cut(out_weight, FORWARD)]
    own = dot(mine, out_weight)
    context_rows = transposed_context(context, mp)
    got, own, context_rows = lax.optimization_barrier((got, own, context_rows))
    upstream = lax.dynamic_slice_in_dim(cotangent, mp * half, half, 0).astype(F32)

    attn = own + jnp.concatenate(got, 1).astype(F32)
    inverse = lax.rsqrt(jnp.mean(attn * attn, axis=-1, keepdims=True) + norm_floor)
    normed = attn * inverse
    scaled = upstream * norm_gain
    product = jnp.mean(scaled * normed, axis=-1, keepdims=True)
    mine = [
        (inverse * (part - norm * product)).astype(BF)
        for part, norm in zip(cut(scaled, WIDTHS), cut(normed, WIDTHS))
    ]
    gain = jnp.pad(jnp.sum(upstream * normed, axis=0), (0, 512)).reshape(4, -1)

    def back(parts, *others):
        grads = jnp.concatenate([after(part, *others) for part in parts], 1)
        return lax.dot_general(
            grads, out_weight, (((1,), (1,)), ((), ())), preferred_element_type=F32
        ).astype(BF)

    gains = packed(gain)
    wide = gains.shape[1]
    ahead = jnp.pad(gains, ((0, 0), (0, WIDTHS[0] - wide)))
    mine_sent = [jnp.concatenate([mine[0], ahead], 0), mine[1]]
    theirs, near = [], []
    for part in mine_sent:
        theirs.append(moved(part, MP, SWAP))
        near.append(moved(part, C, SWAP))
    back_mine = back(mine)
    theirs[0] = after(theirs[0], back_mine)

    def begin(k, parts):
        parts_k = [mine_sent[k], theirs[k], near[k], moved(theirs[k], C, SWAP)]
        grads = jnp.concatenate([part[:half] for part in parts_k], 0)
        columns = cut(grads, [grads.shape[1] // 2] * 2)
        sent = {p: dot(context_rows[p][0], c).astype(BF) for p, c in zip(parts, columns)}
        total = None
        if k == 0:
            total = gain + sum(unpacked(part[half:, :wide]) for part in parts_k[1:])
        kept = {p: dot(context_rows[p][1], c) for p, c in zip(parts, columns)}
        return sent, kept, total

    def send(stage, sent, gain=None):
        arrived = {}
        for p, rows in sent.items():
            if p == "a":
                rows = jnp.concatenate([rows, packed(gain)], 0)
            arrived[p] = moved(rows, *ROUTES[p][stage])
        return arrived

    def received(kept, arrived, gain=None):
        sums = {p: kept[p] + arrived[p][: kept[p].shape[0]].astype(F32) for p in kept}
        if gain is not None:
            gain = gain + unpacked(arrived["a"][kept["a"].shape[0] :])
        return sums, gain

    def split(sums):
        sent, kept = {}, {}
        for p, rows in sums.items():
            count = rows.shape[0] // 2
            kept[p], sent[p] = rows[:count], rows[count:].astype(BF)
        return sent, kept

    sent, kept_ab, gain = begin(0, "ab")
    first_ab = send(0, sent, gain)
    sent, kept_cd, _ = begin(1, "cd")
    first_cd = send(0, sent)
    first_ab = {p: after(rows, *kept_cd.values(), *kept_ab.values()) for p, rows in first_ab.items()}
    sums, gain = received(kept_ab, first_ab, gain)
    sent, kept_ab = split(sums)
    second_ab = send(1, sent, gain)
    sums, gain = received(kept_ab, second_ab, gain)
    sent, kept_ab = split(sums)
    third_ab = send(2, sent, gain)
    first_cd = {p: after(rows, *sent.values()) for p, rows in first_cd.items()}
    sums, _ = received(kept_cd, first_cd)
    sent, kept_cd = split(sums)
    second_cd = send(1, sent)
    third_ab = {p: after(rows, *sent.values()) for p, rows in third_ab.items()}
    sums, gain = received(kept_ab, third_ab, gain)

    def owned(parts):
        return lax.all_to_all(
            jnp.concatenate(parts, -1), (QUAD, YL), split_axis=0, concat_axis=0, tiled=True
        )

    tiles = [rows.astype(BF).reshape(8, 8, -1) for rows in sums.values()]
    tiles_ab = owned([*tiles, jnp.broadcast_to(packed(gain), (8, 8, wide))])
    sums, _ = received(kept_cd, second_cd)
    sent, kept_cd = split(sums)
    third_cd = send(2, sent)
    sums, _ = received(kept_cd, third_cd)
    tiles = [rows.astype(BF).reshape(8, 8, -1) for rows in sums.values()]
    tiles_cd = owned(tiles)
    back_theirs = back([theirs[0][:half], theirs[1]], *tiles)
    tiles_cd, back_theirs = lax.optimization_barrier((tiles_cd, back_theirs))
    grad_gain = unpacked(tiles_ab[..., WIDTHS[0] :]).sum(0).reshape(-1)[:width]
    grad_shard = jnp.concatenate(
        [tiles_ab[..., : WIDTHS[0]].astype(F32).sum(0), tiles_cd.astype(F32).sum(0)], 1
    )
    pair = jnp.stack([back_mine, back_theirs])
    grad_context = jnp.concatenate([picked(pair, mp), picked(pair, 1 - mp)], 0)

    shard_rows = first_moment.shape[1]
    master = lax.dynamic_slice_in_dim(
        out_weight, lax.axis_index(DP) * shard_rows, shard_rows, 0
    ).astype(F32)[None]
    new_weight, new_first, new_second = adam_update(
        master, first_moment, second_moment, grad_shard[None]
    )
    return (new_weight, new_first, new_second, grad_gain, grad_context)


def solution(mesh):
    finer = Mesh(mesh.devices.reshape(4, 2, 2, 4, 2, mesh.shape["mp"]), (*DP, MP))
    placed = (P(DP, MP), P(MP, None), P(DP, None), P(), P(MP, DP, None), P(MP, DP, None))
    return jax.shard_map(
        per_device,
        mesh=finer,
        in_specs=placed,
        out_specs=(P(MP, DP, None), P(MP, DP, None), P(MP, DP, None), P(), P(DP, MP)),
        check_vma=False,
    )
```

```python
import jax
import jax.numpy as jnp
from jax import lax
from jax.experimental import pallas as pl
from jax.experimental.pallas import tpu as pltpu
from jax.sharding import Mesh
from jax.sharding import PartitionSpec as P


DP = ("z_1", "z_0", "y_0", "x", "core")
QUAD, PARITY, YL, X, C = DP
Z = (QUAD, PARITY)
MP = "mp"

norm_floor = 0.1
learn_rate = 0.01
beta_one = 0.9
beta_two = 0.95
adam_floor = 1e-08

FORWARD = (1024, 2560)
WIDTHS = (2304, 1280)
ROWS = 32
BF = jnp.bfloat16
F32 = jnp.float32
SWAP = [(0, 1), (1, 0)]
NEAR = (X, [(i, i ^ 1) for i in range(4)])
FAR = (X, [(i, 3 - i) for i in range(4)])
EVEN = (Z, [(i, i ^ 1) for i in range(8)])
ODD = (Z, [(i, (i + 2 * (i % 2) - 1) % 8) for i in range(8)])
ROUTES = {"a": (NEAR, EVEN, FAR), "b": (FAR, ODD, NEAR), "c": (EVEN, NEAR, FAR), "d": (ODD, FAR, NEAR)}


def dot(a, b):
    return jnp.dot(a, b, preferred_element_type=F32)


def picked(array, index):
    return lax.dynamic_index_in_dim(array, index, 0, keepdims=False)


def after(value, *others):
    return lax.optimization_barrier((value, *others))[0]


def moved(value, axis, pairs):
    return lax.ppermute(value, axis, pairs)


def cut(array, widths):
    begin, pieces = 0, []
    for size in widths:
        pieces.append(array[:, begin : begin + size])
        begin += size
    return pieces


def transposed_context(context, mp):
    half = context.shape[0] // 2
    core, x, parity = lax.axis_index(C), lax.axis_index(X), lax.axis_index(PARITY)
    halves = context.reshape(2, half, -1)
    ordered = jnp.concatenate([picked(halves, mp), picked(halves, 1 - mp)], 0)
    rows = ordered.T.reshape(4, 2, 2, 4, 2, 8, 2 * half).transpose(4, 3, 1, 0, 2, 5, 6)
    other = moved(picked(rows, 1 - core), C, SWAP)
    rows = jnp.concatenate([picked(rows, core), other], -1).reshape(4, 2, 64, 2 * 2 * half)

    def block(owner, same):
        return picked(picked(rows, owner), parity if same else 1 - parity)

    at, near, far, across = x, x ^ 1, 3 - x, 3 - (x ^ 1)
    places = {
        "a": ([(near, 1), (across, 1), (near, 0), (across, 0)], [(at, 1), (far, 1), (at, 0), (far, 0)]),
        "b": ([(far, 1), (across, 1), (far, 0), (across, 0)], [(at, 1), (near, 1), (at, 0), (near, 0)]),
        "c": tuple([(owner, same) for owner in (at, far, near, across)] for same in (0, 1)),
        "d": tuple([(owner, same) for owner in (at, near, far, across)] for same in (0, 1)),
    }
    return {
        part: [jnp.concatenate([block(*place) for place in side], 0) for side in sides]
        for part, sides in places.items()
    }


def packed(gain):
    high = lax.reduce_precision(gain, 8, 7)
    return jnp.concatenate([high, gain - high], 0).astype(BF)


def unpacked(rows):
    rows = rows.astype(F32)
    return rows[..., :4, :] + rows[..., 4:, :]


def norm_kernel(mp_ref, own_ref, first_ref, second_ref, cotangent_ref, gain_ref, *outs):
    ahead_ref, behind_ref, sums_ref = outs
    width = own_ref.shape[1]
    parts = ((0, FORWARD[0], first_ref), (FORWARD[0], width, second_ref))
    total = jnp.zeros(sums_ref.shape, F32)
    for row in range(0, ROWS, 8):
        rows = slice(row, row + 8)
        attn = jnp.concatenate(
            [own_ref[rows, low:high] + ref[rows, :].astype(F32) for low, high, ref in parts], 1
        )
        square = jnp.sum(attn * attn, axis=1, keepdims=True) / width
        inverse = lax.rsqrt(square + norm_floor)
        normed = attn * inverse
        upstream = cotangent_ref[rows, :].astype(F32)
        scaled = upstream * gain_ref[...]
        product = jnp.sum(scaled * normed, axis=1, keepdims=True) / width
        grads = (inverse * (scaled - normed * product)).astype(BF)
        ahead_ref[rows, :] = grads[:, : WIDTHS[0]]
        behind_ref[rows, :] = grads[:, WIDTHS[0] :]
        total += upstream * normed

    @pl.when(pl.program_id(0) == 0)
    def _():
        sums_ref[...] = total

    @pl.when(pl.program_id(0) > 0)
    def _():
        sums_ref[...] += total


def norm_backward(mp, own, got, cotangent, norm_gain):
    count, width = own.shape
    steps = count // ROWS

    def block(size):
        return pl.BlockSpec((ROWS, size), lambda i, mp_ref: (i, 0))

    def whole(rows):
        return pl.BlockSpec((rows, width), lambda i, mp_ref: (0, 0))

    return pl.pallas_call(
        norm_kernel,
        grid_spec=pltpu.PrefetchScalarGridSpec(
            num_scalar_prefetch=1,
            grid=(steps,),
            in_specs=[
                block(width),
                *map(block, FORWARD),
                pl.BlockSpec((ROWS, width), lambda i, mp_ref: (mp_ref[0] * steps + i, 0)),
                whole(1),
            ],
            out_specs=[*map(block, WIDTHS), whole(8)],
        ),
        out_shape=[
            *(jax.ShapeDtypeStruct((count, size), BF) for size in WIDTHS),
            jax.ShapeDtypeStruct((8, width), F32),
        ],
        cost_estimate=pl.CostEstimate(
            flops=20 * count * width, transcendentals=count, bytes_accessed=10 * count * width
        ),
    )(mp.reshape(1), own, *got, cotangent, norm_gain.reshape(1, width))


def adam_update(master, first_moment, second_moment, grad_shard):
    new_first = beta_one * first_moment + (1.0 - beta_one) * grad_shard
    new_second = beta_two * second_moment + (1.0 - beta_two) * grad_shard * grad_shard
    new_weight = (master - learn_rate * new_first / (jnp.sqrt(new_second) + adam_floor)).astype(BF)
    return (new_weight, new_first, new_second)


def per_device(context, out_weight, cotangent, norm_gain, first_moment, second_moment):
    tokens, width = cotangent.shape
    half = tokens // 2
    mp = lax.axis_index(MP)
    mine = lax.dynamic_slice_in_dim(context, mp * half, half, 0)
    theirs = lax.dynamic_slice_in_dim(context, (1 - mp) * half, half, 0)
    got = [moved(dot(theirs, columns).astype(BF), MP, SWAP) for columns in cut(out_weight, FORWARD)]
    own = dot(mine, out_weight)
    context_rows = transposed_context(context, mp)
    got, own, context_rows = lax.optimization_barrier((got, own, context_rows))
    *mine, sums = norm_backward(mp, own, got, cotangent, norm_gain)
    gain = sums.sum(0).reshape(4, -1)

    def back(parts, *others):
        grads = jnp.concatenate([after(part, *others) for part in parts], 1)
        return lax.dot_general(
            grads, out_weight, (((1,), (1,)), ((), ())), preferred_element_type=F32
        ).astype(BF)

    wide = gain.shape[1]

    def with_gain(rows, gain):
        spare = ((0, 0), (0, rows.shape[1] - wide))
        return jnp.concatenate([rows, jnp.pad(packed(gain), spare)], 0)

    mine_sent = [with_gain(mine[0], gain), mine[1]]
    theirs, near = [], []
    for part in mine_sent:
        theirs.append(moved(part, MP, SWAP))
        near.append(moved(part, C, SWAP))
    back_mine = back(mine)
    theirs[0] = after(theirs[0], back_mine)

    def begin(k, parts):
        parts_k = [mine_sent[k], theirs[k], near[k], moved(theirs[k], C, SWAP)]
        grads = jnp.concatenate([part[:half] for part in parts_k], 0)
        columns = cut(grads, [grads.shape[1] // 2] * 2)
        sent = {p: dot(context_rows[p][0], c).astype(BF) for p, c in zip(parts, columns)}
        total = None
        if k == 0:
            total = gain + sum(unpacked(part[half:, :wide]) for part in parts_k[1:])
        kept = {p: dot(context_rows[p][1], c) for p, c in zip(parts, columns)}
        return sent, kept, total

    def send(stage, sent, gain=None):
        arrived = {}
        for p, rows in sent.items():
            if p == "a":
                rows = with_gain(rows, gain)
            arrived[p] = moved(rows, *ROUTES[p][stage])
        return arrived

    def received(kept, arrived, gain=None):
        sums = {p: kept[p] + arrived[p][: kept[p].shape[0]].astype(F32) for p in kept}
        if gain is not None:
            gain = gain + unpacked(arrived["a"][kept["a"].shape[0] :, :wide])
        return sums, gain

    def split(sums):
        sent, kept = {}, {}
        for p, rows in sums.items():
            count = rows.shape[0] // 2
            kept[p], sent[p] = rows[:count], rows[count:].astype(BF)
        return sent, kept

    sent, kept, gain = begin(0, "ab")
    first = send(0, sent, gain)
    theirs[1], near[1] = (after(part, *kept.values()) for part in (theirs[1], near[1]))
    sent, kept_cd, _ = begin(1, "cd")
    first |= send(0, sent)
    kept |= kept_cd
    first = {p: after(rows, *kept.values()) for p, rows in first.items()}
    sums, gain = received(kept, first, gain)
    sent, kept = split(sums)
    sums, gain = received(kept, send(1, sent, gain), gain)
    sent, kept = split(sums)
    sums, gain = received(kept, send(2, sent, gain), gain)
    tiles = [rows.astype(BF).reshape(8, 8, -1) for rows in sums.values()]
    tiles.append(jnp.broadcast_to(packed(gain), (8, 8, wide)))
    tiles = lax.all_to_all(
        jnp.concatenate(tiles, -1), (QUAD, YL), split_axis=0, concat_axis=0, tiled=True
    )
    back_theirs = back([theirs[0][:half], theirs[1]], *sums.values())
    tiles, back_theirs = lax.optimization_barrier((tiles, back_theirs))
    grad_gain = unpacked(tiles[..., width:]).sum(0).reshape(-1)
    grad_shard = tiles[..., :width].astype(F32).sum(0)
    pair = jnp.stack([back_mine, back_theirs])
    grad_context = jnp.concatenate([picked(pair, mp), picked(pair, 1 - mp)], 0)

    shard_rows = first_moment.shape[1]
    master = lax.dynamic_slice_in_dim(
        out_weight, lax.axis_index(DP) * shard_rows, shard_rows, 0
    ).astype(F32)[None]
    new_weight, new_first, new_second = adam_update(
        master, first_moment, second_moment, grad_shard[None]
    )
    return (new_weight, new_first, new_second, grad_gain, grad_context)


def solution(mesh):
    finer = Mesh(mesh.devices.reshape(4, 2, 2, 4, 2, mesh.shape["mp"]), (*DP, MP))
    placed = (P(DP, MP), P(MP, None), P(DP, None), P(), P(MP, DP, None), P(MP, DP, None))
    return jax.shard_map(
        per_device,
        mesh=finer,
        in_specs=placed,
        out_specs=(P(MP, DP, None), P(MP, DP, None), P(MP, DP, None), P(), P(DP, MP)),
        check_vma=False,
    )
```

```python
import jax
import jax.numpy as jnp
from jax import lax
from jax.sharding import Mesh
from jax.sharding import PartitionSpec as P


DP = ("z_1", "z_0", "y_0", "x", "core")
QUAD, PARITY, YL, X, C = DP
Z = (QUAD, PARITY)
MP = "mp"

norm_floor = 0.1
learn_rate = 0.01
beta_one = 0.9
beta_two = 0.95
adam_floor = 1e-08

AHEAD = 240
FORWARD = (1024, 2560)
PARTS = "abcd"
BF = jnp.bfloat16
F32 = jnp.float32
SWAP = [(0, 1), (1, 0)]
NEAR = (X, [(i, i ^ 1) for i in range(4)])
FAR = (X, [(i, 3 - i) for i in range(4)])
EVEN = (Z, [(i, i ^ 1) for i in range(8)])
ODD = (Z, [(i, (i + 2 * (i % 2) - 1) % 8) for i in range(8)])
ROUTES = {"a": (NEAR, EVEN, FAR), "b": (FAR, ODD, NEAR), "c": (EVEN, NEAR, FAR), "d": (ODD, FAR, NEAR)}


def dot(a, b):
    return jnp.dot(a, b, preferred_element_type=F32)


def picked(array, index):
    return lax.dynamic_index_in_dim(array, index, 0, keepdims=False)


def after(value, *others):
    return lax.optimization_barrier((value, *others))[0]


def moved(value, axis, pairs):
    return lax.ppermute(value, axis, pairs)


def cut(array, widths):
    begin, pieces = 0, []
    for size in widths:
        pieces.append(array[:, begin : begin + size])
        begin += size
    return pieces


def transposed_context(context):
    tokens = context.shape[0]
    core, x, parity = lax.axis_index(C), lax.axis_index(X), lax.axis_index(PARITY)
    rows = context.T.reshape(4, 2, 2, 4, 2, 8, tokens).transpose(4, 3, 1, 0, 2, 5, 6)
    other = moved(picked(rows, 1 - core), C, SWAP)
    rows = jnp.concatenate([picked(rows, core), other], -1).reshape(4, 2, 64, 2 * tokens)

    def block(owner, same):
        return picked(picked(rows, owner), parity if same else 1 - parity)

    at, near, far, across = x, x ^ 1, 3 - x, 3 - (x ^ 1)
    places = {
        "a": ([(near, 1), (across, 1), (near, 0), (across, 0)], [(at, 1), (far, 1), (at, 0), (far, 0)]),
        "b": ([(far, 1), (across, 1), (far, 0), (across, 0)], [(at, 1), (near, 1), (at, 0), (near, 0)]),
        "c": tuple([(owner, same) for owner in (at, far, near, across)] for same in (0, 1)),
        "d": tuple([(owner, same) for owner in (at, near, far, across)] for same in (0, 1)),
    }
    return {
        part: [jnp.concatenate([block(*place) for place in side], 0) for side in sides]
        for part, sides in places.items()
    }


def packed(gain):
    high = lax.reduce_precision(gain, 8, 7)
    return jnp.concatenate([high, gain - high], 0).astype(BF)


def unpacked(rows):
    rows = rows.astype(F32)
    return rows[..., :4, :] + rows[..., 4:, :]


def adam_update(master, first_moment, second_moment, grad_shard):
    new_first = beta_one * first_moment + (1.0 - beta_one) * grad_shard
    new_second = beta_two * second_moment + (1.0 - beta_two) * grad_shard * grad_shard
    new_weight = (master - learn_rate * new_first / (jnp.sqrt(new_second) + adam_floor)).astype(BF)
    return (new_weight, new_first, new_second)


def per_device(context, out_weight, cotangent, norm_gain, first_moment, second_moment):
    tokens, width = cotangent.shape
    ahead, behind = slice(0, AHEAD), slice(AHEAD, tokens)

    def partial(rows, columns):
        own = dot(context[rows], columns).astype(BF)
        return own, moved(own, MP, SWAP)

    first, second = cut(out_weight, FORWARD)
    pieces = [partial(ahead, first), partial(ahead, second), partial(behind, out_weight)]
    context_rows = transposed_context(context)

    def norm_backward(rows, *pieces):
        attn = jnp.concatenate([own.astype(F32) + got.astype(F32) for own, got in pieces], 1)
        inverse = lax.rsqrt(jnp.mean(attn * attn, axis=-1, keepdims=True) + norm_floor)
        normed = attn * inverse
        upstream = cotangent[rows].astype(F32)
        scaled = upstream * norm_gain
        product = jnp.mean(scaled * normed, axis=-1, keepdims=True)
        grads = (inverse * (scaled - normed * product)).astype(BF)
        return grads, jnp.sum(upstream * normed, axis=0)

    context_rows, pieces[1] = lax.optimization_barrier((context_rows, pieces[1]))
    grads_ahead, gain_ahead = norm_backward(ahead, *pieces[:2])
    near_ahead = moved(grads_ahead, C, SWAP)
    near_ahead, pieces[2], gain_ahead = lax.optimization_barrier(
        (near_ahead, pieces[2], gain_ahead)
    )
    grads_behind, gain_behind = norm_backward(behind, pieces[2])
    near_behind = moved(grads_behind, C, SWAP)
    gain = gain_ahead + gain_behind
    near_gain = moved(gain, C, SWAP)

    grads = jnp.concatenate([grads_ahead, grads_behind, near_ahead, near_behind], 0)
    columns = dict(zip(PARTS, cut(grads, [width // 4] * 4)))
    sent = {}
    for p in PARTS:
        sent[p] = dot(context_rows[p][0], columns[p]).astype(BF)
    gain = (gain + after(near_gain, *sent.values())).reshape(4, -1)
    kept = {p: dot(context_rows[p][1], columns[p]) for p in PARTS}

    def send(stage, sent, gain):
        arrived = {}
        for p, rows in sent.items():
            if p == PARTS[-1]:
                rows = jnp.concatenate([rows, packed(gain)], 0)
            arrived[p] = moved(rows, *ROUTES[p][stage])
        return arrived

    def received(kept, arrived, gain):
        sums = {p: kept[p] + arrived[p][: kept[p].shape[0]].astype(F32) for p in PARTS}
        return sums, gain + unpacked(arrived[PARTS[-1]][kept[PARTS[-1]].shape[0] :])

    def split(sums):
        sent, kept = {}, {}
        for p, rows in sums.items():
            count = rows.shape[0] // 2
            kept[p], sent[p] = rows[:count], rows[count:].astype(BF)
        return sent, kept

    arrived = send(0, sent, gain)
    arrived = {p: after(rows, *kept.values()) for p, rows in arrived.items()}
    sums, gain = received(kept, arrived, gain)
    sent, kept = split(sums)
    sums, gain = received(kept, send(1, sent, gain), gain)
    sent, kept = split(sums)
    arrived = lax.optimization_barrier(send(2, sent, gain))
    sums, gain = received(kept, arrived, gain)
    tiles = [rows.astype(BF).reshape(8, 8, -1) for rows in sums.values()]
    *tiles, gains = lax.optimization_barrier((*tiles, packed(gain)))
    tiles.append(jnp.broadcast_to(gains, (8, *gains.shape)))
    tiles = jnp.concatenate(tiles, -1)
    arrived = lax.all_to_all(tiles, (QUAD, YL), split_axis=0, concat_axis=0, tiled=True)
    grads = [after(part, tiles) for part in (grads_ahead, grads_behind)]
    grad_context = lax.dot_general(
        jnp.concatenate(grads, 0),
        out_weight,
        (((1,), (1,)), ((), ())),
        preferred_element_type=F32,
    ).astype(BF)
    tiles, grad_context = lax.optimization_barrier((arrived, grad_context))
    grad_gain = unpacked(tiles[..., width:]).sum(0).reshape(-1)
    grad_shard = tiles[..., :width].astype(F32).sum(0)

    shard_rows = first_moment.shape[1]
    master = lax.dynamic_slice_in_dim(
        out_weight, lax.axis_index(DP) * shard_rows, shard_rows, 0
    ).astype(F32)[None]
    new_weight, new_first, new_second = adam_update(
        master, first_moment, second_moment, grad_shard[None]
    )
    return (new_weight, new_first, new_second, grad_gain, grad_context)


def solution(mesh):
    finer = Mesh(mesh.devices.reshape(4, 2, 2, 4, 2, mesh.shape["mp"]), (*DP, MP))
    placed = (P(DP, MP), P(MP, None), P(DP, None), P(), P(MP, DP, None), P(MP, DP, None))
    return jax.shard_map(
        per_device,
        mesh=finer,
        in_specs=placed,
        out_specs=(P(MP, DP, None), P(MP, DP, None), P(MP, DP, None), P(), P(DP, MP)),
        check_vma=False,
    )
```

```python
import jax
import jax.numpy as jnp
from jax import lax
from jax.sharding import Mesh
from jax.sharding import PartitionSpec as P


DP = ("z_1", "z_0", "y_0", "x", "core")
QUAD, PARITY, YL, X, C = DP
Z = (QUAD, PARITY)
MP = "mp"

norm_floor = 0.1
learn_rate = 0.01
beta_one = 0.9
beta_two = 0.95
adam_floor = 1e-08

AHEAD = 240
FORWARD = (1024, 2560)
PARTS = "abcd"
BF = jnp.bfloat16
F32 = jnp.float32
SWAP = [(0, 1), (1, 0)]
NEAR = (X, [(i, i ^ 1) for i in range(4)])
FAR = (X, [(i, 3 - i) for i in range(4)])
EVEN = (Z, [(i, i ^ 1) for i in range(8)])
ODD = (Z, [(i, (i + 2 * (i % 2) - 1) % 8) for i in range(8)])
ROUTES = {"a": (NEAR, EVEN, FAR), "b": (FAR, ODD, NEAR), "c": (EVEN, NEAR, FAR), "d": (ODD, FAR, NEAR)}


def dot(a, b):
    return jnp.dot(a, b, preferred_element_type=F32)


def picked(array, index):
    return lax.dynamic_index_in_dim(array, index, 0, keepdims=False)


def after(value, *others):
    return lax.optimization_barrier((value, *others))[0]


def moved(value, axis, pairs):
    return lax.ppermute(value, axis, pairs)


def cut(array, widths):
    begin, pieces = 0, []
    for size in widths:
        pieces.append(array[:, begin : begin + size])
        begin += size
    return pieces


def transposed_context(context):
    tokens = context.shape[0]
    core, x, parity = lax.axis_index(C), lax.axis_index(X), lax.axis_index(PARITY)
    rows = context.T.reshape(4, 2, 2, 4, 2, 8, tokens).transpose(4, 3, 1, 0, 2, 5, 6)
    other = moved(picked(rows, 1 - core), C, SWAP)
    rows = jnp.concatenate([picked(rows, core), other], -1).reshape(4, 2, 64, 2 * tokens)

    def block(owner, same):
        return picked(picked(rows, owner), parity if same else 1 - parity)

    at, near, far, across = x, x ^ 1, 3 - x, 3 - (x ^ 1)
    places = {
        "a": ([(near, 1), (across, 1), (near, 0), (across, 0)], [(at, 1), (far, 1), (at, 0), (far, 0)]),
        "b": ([(far, 1), (across, 1), (far, 0), (across, 0)], [(at, 1), (near, 1), (at, 0), (near, 0)]),
        "c": tuple([(owner, same) for owner in (at, far, near, across)] for same in (0, 1)),
        "d": tuple([(owner, same) for owner in (at, near, far, across)] for same in (0, 1)),
    }
    return {
        part: [jnp.concatenate([block(*place) for place in side], 0) for side in sides]
        for part, sides in places.items()
    }


def packed(gain):
    high = lax.reduce_precision(gain, 8, 7)
    return jnp.concatenate([high, gain - high], 0).astype(BF)


def unpacked(rows):
    rows = rows.astype(F32)
    return rows[..., :4, :] + rows[..., 4:, :]


def adam_update(master, first_moment, second_moment, grad_shard):
    new_first = beta_one * first_moment + (1.0 - beta_one) * grad_shard
    new_second = beta_two * second_moment + (1.0 - beta_two) * grad_shard * grad_shard
    new_weight = (master - learn_rate * new_first / (jnp.sqrt(new_second) + adam_floor)).astype(BF)
    return (new_weight, new_first, new_second)


def per_device(context, out_weight, cotangent, norm_gain, first_moment, second_moment):
    tokens, width = cotangent.shape
    ahead, behind = slice(0, AHEAD), slice(AHEAD, tokens)

    def partial(rows, columns):
        own = dot(context[rows], columns).astype(BF)
        return own, moved(own, MP, SWAP)

    first, second = cut(out_weight, FORWARD)
    pieces = [partial(ahead, first), partial(ahead, second), partial(behind, out_weight)]
    context_rows = transposed_context(context)

    def norm_backward(rows, *pieces):
        attn = jnp.concatenate([own.astype(F32) + got.astype(F32) for own, got in pieces], 1)
        inverse = lax.rsqrt(jnp.mean(attn * attn, axis=-1, keepdims=True) + norm_floor)
        normed = attn * inverse
        upstream = cotangent[rows].astype(F32)
        scaled = upstream * norm_gain
        product = jnp.mean(scaled * normed, axis=-1, keepdims=True)
        grads = (inverse * (scaled - normed * product)).astype(BF)
        return grads, jnp.sum(upstream * normed, axis=0)

    context_rows, pieces[1] = lax.optimization_barrier((context_rows, pieces[1]))
    grads_ahead, gain_ahead = norm_backward(ahead, *pieces[:2])
    near_ahead = moved(grads_ahead, C, SWAP)
    near_ahead, pieces[2], gain_ahead = lax.optimization_barrier(
        (near_ahead, pieces[2], gain_ahead)
    )
    grads_behind, gain_behind = norm_backward(behind, pieces[2])
    near_behind = moved(grads_behind, C, SWAP)
    gain = gain_ahead + gain_behind
    near_gain = moved(gain, C, SWAP)

    everyone = (grads_ahead, grads_behind, near_ahead, near_behind)
    columns, sent, kept = {}, {}, {}
    for k, p in enumerate(PARTS):
        cols = slice(k * width // 4, (k + 1) * width // 4)
        columns[p] = jnp.concatenate([part[:, cols] for part in everyone], 0)
        columns[p] = lax.optimization_barrier(columns[p])
        sent[p] = dot(context_rows[p][0], columns[p]).astype(BF)
    gain = (gain + after(near_gain, *sent.values())).reshape(4, -1)
    for p in PARTS:
        kept[p] = dot(context_rows[p][1], columns[p])

    def send(stage, sent, gain):
        arrived = {}
        for p, rows in sent.items():
            if p == PARTS[-1]:
                rows = jnp.concatenate([rows, packed(gain)], 0)
            arrived[p] = moved(rows, *ROUTES[p][stage])
        return arrived

    def received(kept, arrived, gain):
        sums = {p: kept[p] + arrived[p][: kept[p].shape[0]].astype(F32) for p in PARTS}
        return sums, gain + unpacked(arrived[PARTS[-1]][kept[PARTS[-1]].shape[0] :])

    def split(sums):
        sent, kept = {}, {}
        for p, rows in sums.items():
            count = rows.shape[0] // 2
            kept[p], sent[p] = rows[:count], rows[count:].astype(BF)
        return sent, kept

    arrived = send(0, sent, gain)
    arrived = {p: after(rows, *kept.values()) for p, rows in arrived.items()}
    sums, gain = received(kept, arrived, gain)
    sent, kept = split(sums)
    sums, gain = received(kept, send(1, sent, gain), gain)
    sent, kept = split(sums)

    def joined(first, second, extra):
        rows = jnp.concatenate([sent[first], sent[second]], 1)
        if extra is not None:
            spare = ((0, 0), (0, rows.shape[1] - extra.shape[1]))
            rows = jnp.concatenate([rows, jnp.pad(extra, spare)], 0)
        got = moved(rows, *ROUTES[first][2])
        return jnp.concatenate([kept[first], kept[second]], 1) + got[:64].astype(F32), got[64:]

    left, _ = joined("a", "c", None)
    right, gains = joined("b", "d", packed(gain))
    gain += unpacked(gains[:, : gain.shape[1]])
    left, right, gains = lax.optimization_barrier(
        (left.astype(BF), right.astype(BF), packed(gain))
    )
    tiles = jnp.concatenate(
        [
            left.reshape(8, 8, -1),
            right.reshape(8, 8, -1),
            jnp.broadcast_to(gains, (8, *gains.shape)),
        ],
        -1,
    )
    arrived = lax.all_to_all(tiles, (QUAD, YL), split_axis=0, concat_axis=0, tiled=True)
    grads = [after(part, tiles) for part in (grads_ahead, grads_behind)]
    grad_context = lax.dot_general(
        jnp.concatenate(grads, 0),
        out_weight,
        (((1,), (1,)), ((), ())),
        preferred_element_type=F32,
    ).astype(BF)
    tiles, grad_context = lax.optimization_barrier((arrived, grad_context))
    grad_gain = unpacked(tiles[..., width:]).sum(0).reshape(-1)
    grad_shard = tiles[..., :width].astype(F32).sum(0)
    part_a, part_c, part_b, part_d = cut(grad_shard, [width // 4] * 4)
    grad_shard = jnp.concatenate([part_a, part_b, part_c, part_d], 1)

    shard_rows = first_moment.shape[1]
    master = lax.dynamic_slice_in_dim(
        out_weight, lax.axis_index(DP) * shard_rows, shard_rows, 0
    ).astype(F32)[None]
    new_weight, new_first, new_second = adam_update(
        master, first_moment, second_moment, grad_shard[None]
    )
    return (new_weight, new_first, new_second, grad_gain, grad_context)


def solution(mesh):
    finer = Mesh(mesh.devices.reshape(4, 2, 2, 4, 2, mesh.shape["mp"]), (*DP, MP))
    placed = (P(DP, MP), P(MP, None), P(DP, None), P(), P(MP, DP, None), P(MP, DP, None))
    return jax.shard_map(
        per_device,
        mesh=finer,
        in_specs=placed,
        out_specs=(P(MP, DP, None), P(MP, DP, None), P(MP, DP, None), P(), P(DP, MP)),
        check_vma=False,
    )
```

```python
import jax
import jax.numpy as jnp
from jax import lax
from jax.sharding import Mesh
from jax.sharding import PartitionSpec as P


DP = ("z_1", "z_0", "y_0", "x", "core")
QUAD, PARITY, YL, X, C = DP
Z = (QUAD, PARITY)
MP = "mp"

norm_floor = 0.1
learn_rate = 0.01
beta_one = 0.9
beta_two = 0.95
adam_floor = 1e-08

AHEAD = 240
FORWARD = (1024, 2560)
PARTS = {"a": 1152, "b": 896, "c": 896, "d": 640}
BF = jnp.bfloat16
F32 = jnp.float32
SWAP = [(0, 1), (1, 0)]
NEAR = (X, [(i, i ^ 1) for i in range(4)])
FAR = (X, [(i, 3 - i) for i in range(4)])
EVEN = (Z, [(i, i ^ 1) for i in range(8)])
ODD = (Z, [(i, (i + 2 * (i % 2) - 1) % 8) for i in range(8)])
ROUTES = {"a": (NEAR, EVEN, FAR), "b": (FAR, ODD, NEAR), "c": (EVEN, NEAR, FAR), "d": (ODD, FAR, NEAR)}


def dot(a, b):
    return jnp.dot(a, b, preferred_element_type=F32)


def picked(array, index):
    return lax.dynamic_index_in_dim(array, index, 0, keepdims=False)


def after(value, *others):
    return lax.optimization_barrier((value, *others))[0]


def moved(value, axis, pairs):
    return lax.ppermute(value, axis, pairs)


def cut(array, widths):
    begin, pieces = 0, []
    for size in widths:
        pieces.append(array[:, begin : begin + size])
        begin += size
    return pieces


def transposed_context(context):
    tokens = context.shape[0]
    core, x, parity = lax.axis_index(C), lax.axis_index(X), lax.axis_index(PARITY)
    rows = context.T.reshape(4, 2, 2, 4, 2, 8, tokens).transpose(4, 3, 1, 0, 2, 5, 6)
    other = moved(picked(rows, 1 - core), C, SWAP)
    rows = jnp.concatenate([picked(rows, core), other], -1).reshape(4, 2, 64, 2 * tokens)

    def block(owner, same):
        return picked(picked(rows, owner), parity if same else 1 - parity)

    at, near, far, across = x, x ^ 1, 3 - x, 3 - (x ^ 1)
    places = {
        "a": ([(near, 1), (across, 1), (near, 0), (across, 0)], [(at, 1), (far, 1), (at, 0), (far, 0)]),
        "b": ([(far, 1), (across, 1), (far, 0), (across, 0)], [(at, 1), (near, 1), (at, 0), (near, 0)]),
        "c": tuple([(owner, same) for owner in (at, far, near, across)] for same in (0, 1)),
        "d": tuple([(owner, same) for owner in (at, near, far, across)] for same in (0, 1)),
    }
    return {
        part: [jnp.concatenate([block(*place) for place in side], 0) for side in sides]
        for part, sides in places.items()
    }


def packed(gain):
    high = lax.reduce_precision(gain, 8, 7)
    return jnp.concatenate([high, gain - high], 0).astype(BF)


def unpacked(rows):
    rows = rows.astype(F32)
    return rows[..., :4, :] + rows[..., 4:, :]


def adam_update(master, first_moment, second_moment, grad_shard):
    new_first = beta_one * first_moment + (1.0 - beta_one) * grad_shard
    new_second = beta_two * second_moment + (1.0 - beta_two) * grad_shard * grad_shard
    new_weight = (master - learn_rate * new_first / (jnp.sqrt(new_second) + adam_floor)).astype(BF)
    return (new_weight, new_first, new_second)


def per_device(context, out_weight, cotangent, norm_gain, first_moment, second_moment):
    tokens, width = cotangent.shape
    ahead, behind = slice(0, AHEAD), slice(AHEAD, tokens)

    def partial(rows, columns):
        own = dot(context[rows], columns).astype(BF)
        return own, moved(own, MP, SWAP)

    first, second = cut(out_weight, FORWARD)
    pieces = [partial(ahead, first), partial(ahead, second), partial(behind, out_weight)]
    context_rows = transposed_context(context)

    def norm_backward(rows, *pieces):
        attn = jnp.concatenate([own.astype(F32) + got.astype(F32) for own, got in pieces], 1)
        inverse = lax.rsqrt(jnp.mean(attn * attn, axis=-1, keepdims=True) + norm_floor)
        normed = attn * inverse
        upstream = cotangent[rows].astype(F32)
        scaled = upstream * norm_gain
        product = jnp.mean(scaled * normed, axis=-1, keepdims=True)
        grads = (inverse * (scaled - normed * product)).astype(BF)
        return grads, jnp.sum(upstream * normed, axis=0)

    context_rows, pieces[1] = lax.optimization_barrier((context_rows, pieces[1]))
    grads_ahead, gain_ahead = norm_backward(ahead, *pieces[:2])
    near_ahead = moved(grads_ahead, C, SWAP)
    near_ahead, pieces[2], gain_ahead = lax.optimization_barrier(
        (near_ahead, pieces[2], gain_ahead)
    )
    grads_behind, gain_behind = norm_backward(behind, pieces[2])
    near_behind = moved(grads_behind, C, SWAP)
    gain = gain_ahead + gain_behind
    near_gain = moved(gain, C, SWAP)

    everyone = (grads_ahead, grads_behind, near_ahead, near_behind)
    whole = [dict(zip(PARTS, cut(part, PARTS.values()))) for part in everyone]
    columns, sent = {}, {}
    for p in PARTS:
        columns[p] = jnp.concatenate([part[p] for part in whole], 0)
        columns[p] = lax.optimization_barrier(columns[p])
        sent[p] = dot(context_rows[p][0], columns[p]).astype(BF)
        if p == "b":
            gain = (gain + after(near_gain, *sent.values())).reshape(4, -1)

    def with_gain(rows):
        spare = ((0, 0), (0, rows.shape[1] - gain.shape[1]))
        return jnp.concatenate([rows, jnp.pad(packed(gain), spare)], 0)

    def product(p, rows):
        return dot(context_rows[p][1][rows], columns[p])

    low, high = slice(0, 128), slice(128, 256)
    sent["c"] = with_gain(sent["c"])
    first = {p: moved(rows, *ROUTES[p][0]) for p, rows in sent.items()}
    second, kept = {}, {}
    gain += unpacked(first["c"][256:])
    for p in PARTS:
        rows = (product(p, high) + first[p][high].astype(F32)).astype(BF)
        second[p] = moved(with_gain(rows) if p == "c" else rows, *ROUTES[p][1])
    for p in PARTS:
        kept[p] = product(p, low) + first[p][low].astype(F32)
    gain += unpacked(second["c"][128:])

    def joined(one, other, wrap):
        parts = (one, other)
        rows = [kept[p][64:] + second[p][64:128].astype(F32) for p in parts]
        rows = wrap(jnp.concatenate(rows, 1).astype(BF))
        got = moved(rows, *ROUTES[one][2])
        rows = [kept[p][:64] + second[p][:64].astype(F32) for p in parts]
        return jnp.concatenate(rows, 1) + got[:64].astype(F32), got[64:]

    left, gains = joined("a", "c", with_gain)
    right, _ = joined("b", "d", lambda rows: rows)
    gain += unpacked(gains[:, : gain.shape[1]])
    left, right, gains = lax.optimization_barrier(
        (left.astype(BF), right.astype(BF), packed(gain))
    )
    tiles = jnp.concatenate(
        [
            left.reshape(8, 8, -1),
            right.reshape(8, 8, -1),
            jnp.broadcast_to(gains, (8, *gains.shape)),
        ],
        -1,
    )
    arrived = lax.all_to_all(tiles, (QUAD, YL), split_axis=0, concat_axis=0, tiled=True)
    grads = [after(part, tiles) for part in (grads_ahead, grads_behind)]
    grad_context = lax.dot_general(
        jnp.concatenate(grads, 0),
        out_weight,
        (((1,), (1,)), ((), ())),
        preferred_element_type=F32,
    ).astype(BF)
    tiles, grad_context = lax.optimization_barrier((arrived, grad_context))
    grad_gain = unpacked(tiles[..., width:]).sum(0).reshape(-1)
    grad_shard = tiles[..., :width].astype(F32).sum(0)
    part_a, part_c, part_b, part_d = cut(grad_shard, [PARTS[p] for p in "acbd"])
    grad_shard = jnp.concatenate([part_a, part_b, part_c, part_d], 1)

    shard_rows = first_moment.shape[1]
    master = lax.dynamic_slice_in_dim(
        out_weight, lax.axis_index(DP) * shard_rows, shard_rows, 0
    ).astype(F32)[None]
    new_weight, new_first, new_second = adam_update(
        master, first_moment, second_moment, grad_shard[None]
    )
    return (new_weight, new_first, new_second, grad_gain, grad_context)


def solution(mesh):
    finer = Mesh(mesh.devices.reshape(4, 2, 2, 4, 2, mesh.shape["mp"]), (*DP, MP))
    placed = (P(DP, MP), P(MP, None), P(DP, None), P(), P(MP, DP, None), P(MP, DP, None))
    return jax.shard_map(
        per_device,
        mesh=finer,
        in_specs=placed,
        out_specs=(P(MP, DP, None), P(MP, DP, None), P(MP, DP, None), P(), P(DP, MP)),
        check_vma=False,
    )
```

```python
import jax
import jax.numpy as jnp
from jax import lax
from jax.sharding import Mesh
from jax.sharding import PartitionSpec as P


DP = ("z_1", "z_0", "y_0", "x", "core")
QUAD, PARITY, YL, X, C = DP
Z = (QUAD, PARITY)
MP = "mp"

norm_floor = 0.1
learn_rate = 0.01
beta_one = 0.9
beta_two = 0.95
adam_floor = 1e-08

AHEAD = 240
FORWARD = (768, 2816)
PARTS = dict.fromkeys("abcd", 896)
BF = jnp.bfloat16
F32 = jnp.float32
SWAP = [(0, 1), (1, 0)]
NEAR = (X, [(i, i ^ 1) for i in range(4)])
FAR = (X, [(i, 3 - i) for i in range(4)])
EVEN = (Z, [(i, i ^ 1) for i in range(8)])
ODD = (Z, [(i, (i + 2 * (i % 2) - 1) % 8) for i in range(8)])
ROUTES = {"a": (NEAR, EVEN, FAR), "b": (FAR, ODD, NEAR), "c": (EVEN, NEAR, FAR), "d": (ODD, FAR, NEAR)}


def dot(a, b):
    return jnp.dot(a, b, preferred_element_type=F32)


def picked(array, index):
    return lax.dynamic_index_in_dim(array, index, 0, keepdims=False)


def after(value, *others):
    return lax.optimization_barrier((value, *others))[0]


def moved(value, axis, pairs):
    return lax.ppermute(value, axis, pairs)


def cut(array, widths):
    begin, pieces = 0, []
    for size in widths:
        pieces.append(array[:, begin : begin + size])
        begin += size
    return pieces


def transposed_context(context):
    tokens = context.shape[0]
    core, x, parity = lax.axis_index(C), lax.axis_index(X), lax.axis_index(PARITY)
    rows = context.T.reshape(4, 2, 2, 4, 2, 8, tokens).transpose(4, 3, 1, 0, 2, 5, 6)
    other = moved(picked(rows, 1 - core), C, SWAP)
    rows = jnp.concatenate([picked(rows, core), other], -1).reshape(4, 2, 64, 2 * tokens)

    def block(owner, same):
        return picked(picked(rows, owner), parity if same else 1 - parity)

    at, near, far, across = x, x ^ 1, 3 - x, 3 - (x ^ 1)
    places = {
        "a": ([(near, 1), (across, 1), (near, 0), (across, 0)], [(at, 1), (far, 1), (at, 0), (far, 0)]),
        "b": ([(far, 1), (across, 1), (far, 0), (across, 0)], [(at, 1), (near, 1), (at, 0), (near, 0)]),
        "c": tuple([(owner, same) for owner in (at, far, near, across)] for same in (0, 1)),
        "d": tuple([(owner, same) for owner in (at, near, far, across)] for same in (0, 1)),
    }
    return {
        part: [jnp.concatenate([block(*place) for place in side], 0) for side in sides]
        for part, sides in places.items()
    }


def packed(gain):
    high = lax.reduce_precision(gain, 8, 7)
    return jnp.concatenate([high, gain - high], 0).astype(BF)


def unpacked(rows):
    rows = rows.astype(F32)
    return rows[..., :4, :] + rows[..., 4:, :]


def adam_update(master, first_moment, second_moment, grad_shard):
    new_first = beta_one * first_moment + (1.0 - beta_one) * grad_shard
    new_second = beta_two * second_moment + (1.0 - beta_two) * grad_shard * grad_shard
    new_weight = (master - learn_rate * new_first / (jnp.sqrt(new_second) + adam_floor)).astype(BF)
    return (new_weight, new_first, new_second)


def per_device(context, out_weight, cotangent, norm_gain, first_moment, second_moment):
    tokens, width = cotangent.shape
    ahead, behind = slice(0, AHEAD), slice(AHEAD, tokens)

    def partial(rows, columns):
        own = dot(context[rows], columns).astype(BF)
        return own, moved(own, MP, SWAP)

    first, second = cut(out_weight, FORWARD)
    pieces = [partial(ahead, first), partial(ahead, second), partial(behind, out_weight)]
    context_rows = transposed_context(context)

    def norm_backward(rows, *pieces):
        attn = jnp.concatenate([own.astype(F32) + got.astype(F32) for own, got in pieces], 1)
        inverse = lax.rsqrt(jnp.mean(attn * attn, axis=-1, keepdims=True) + norm_floor)
        normed = attn * inverse
        upstream = cotangent[rows].astype(F32)
        scaled = upstream * norm_gain
        product = jnp.mean(scaled * normed, axis=-1, keepdims=True)
        grads = (inverse * (scaled - normed * product)).astype(BF)
        return grads, jnp.sum(upstream * normed, axis=0)

    context_rows, pieces[1] = lax.optimization_barrier((context_rows, pieces[1]))
    grads_ahead, gain_ahead = norm_backward(ahead, *pieces[:2])
    near_ahead = moved(grads_ahead, C, SWAP)
    near_ahead, pieces[2], gain_ahead = lax.optimization_barrier(
        (near_ahead, pieces[2], gain_ahead)
    )
    grads_behind, gain_behind = norm_backward(behind, pieces[2])
    near_behind = moved(grads_behind, C, SWAP)
    gain = gain_ahead + gain_behind
    near_gain = moved(gain, C, SWAP)

    everyone = (grads_ahead, grads_behind, near_ahead, near_behind)
    whole = [dict(zip(PARTS, cut(part, PARTS.values()))) for part in everyone]
    columns, sent = {}, {}
    for p in PARTS:
        columns[p] = jnp.concatenate([part[p] for part in whole], 0)
        columns[p] = lax.optimization_barrier(columns[p])
        sent[p] = dot(context_rows[p][0], columns[p]).astype(BF)
        if p == "b":
            gain = (gain + after(near_gain, *sent.values())).reshape(4, -1)

    def with_gain(rows):
        spare = ((0, 0), (0, rows.shape[1] - gain.shape[1]))
        return jnp.concatenate([rows, jnp.pad(packed(gain), spare)], 0)

    def product(p, rows):
        return dot(context_rows[p][1][rows], columns[p])

    low, high = slice(0, 128), slice(128, 256)
    sent["c"] = with_gain(sent["c"])
    first = {p: moved(rows, *ROUTES[p][0]) for p, rows in sent.items()}
    second, kept = {}, {}
    for p in PARTS:
        rows = (product(p, high) + first[p][high].astype(F32)).astype(BF)
        if p == "c":
            gain += unpacked(after(first["c"][256:], rows))
        second[p] = moved(with_gain(rows) if p == "c" else rows, *ROUTES[p][1])
    for p in PARTS:
        kept[p] = product(p, low) + first[p][low].astype(F32)
    gain += unpacked(second["c"][128:])

    def joined(one, other, wrap):
        parts = (one, other)
        rows = [kept[p][64:] + second[p][64:128].astype(F32) for p in parts]
        rows = wrap(jnp.concatenate(rows, 1).astype(BF))
        got = moved(rows, *ROUTES[one][2])
        rows = [kept[p][:64] + second[p][:64].astype(F32) for p in parts]
        return jnp.concatenate(rows, 1) + got[:64].astype(F32), got[64:]

    left, gains = joined("a", "c", with_gain)
    right, _ = joined("b", "d", lambda rows: rows)
    gain += unpacked(gains[:, : gain.shape[1]])
    left, right, gains = lax.optimization_barrier(
        (left.astype(BF), right.astype(BF), packed(gain))
    )
    tiles = jnp.concatenate(
        [
            left.reshape(8, 8, -1),
            right.reshape(8, 8, -1),
            jnp.broadcast_to(gains, (8, *gains.shape)),
        ],
        -1,
    )
    arrived = lax.all_to_all(tiles, (QUAD, YL), split_axis=0, concat_axis=0, tiled=True)
    grads = [after(part, tiles) for part in (grads_ahead, grads_behind)]
    grad_context = lax.dot_general(
        jnp.concatenate(grads, 0),
        out_weight,
        (((1,), (1,)), ((), ())),
        preferred_element_type=F32,
    ).astype(BF)
    tiles, grad_context = lax.optimization_barrier((arrived, grad_context))
    grad_gain = unpacked(tiles[..., width:]).sum(0).reshape(-1)
    grad_shard = tiles[..., :width].astype(F32).sum(0)
    part_a, part_c, part_b, part_d = cut(grad_shard, [PARTS[p] for p in "acbd"])
    grad_shard = jnp.concatenate([part_a, part_b, part_c, part_d], 1)

    shard_rows = first_moment.shape[1]
    master = lax.dynamic_slice_in_dim(
        out_weight, lax.axis_index(DP) * shard_rows, shard_rows, 0
    ).astype(F32)[None]
    new_weight, new_first, new_second = adam_update(
        master, first_moment, second_moment, grad_shard[None]
    )
    return (new_weight, new_first, new_second, grad_gain, grad_context)


def solution(mesh):
    finer = Mesh(mesh.devices.reshape(4, 2, 2, 4, 2, mesh.shape["mp"]), (*DP, MP))
    placed = (P(DP, MP), P(MP, None), P(DP, None), P(), P(MP, DP, None), P(MP, DP, None))
    return jax.shard_map(
        per_device,
        mesh=finer,
        in_specs=placed,
        out_specs=(P(MP, DP, None), P(MP, DP, None), P(MP, DP, None), P(), P(DP, MP)),
        check_vma=False,
    )
```

```python
import jax
import jax.numpy as jnp
from jax import lax
from jax.sharding import Mesh
from jax.sharding import PartitionSpec as P


DP = ("z_1", "z_0", "y_0", "x", "core")
QUAD, PARITY, YL, X, C = DP
Z = (QUAD, PARITY)
MP = "mp"

norm_floor = 0.1
learn_rate = 0.01
beta_one = 0.9
beta_two = 0.95
adam_floor = 1e-08

AHEAD = 240
FORWARD = (768, 2816)
PARTS = dict.fromkeys("abcd", 896)
BF = jnp.bfloat16
F32 = jnp.float32
SWAP = [(0, 1), (1, 0)]
NEAR = (X, [(i, i ^ 1) for i in range(4)])
FAR = (X, [(i, 3 - i) for i in range(4)])
EVEN = (Z, [(i, i ^ 1) for i in range(8)])
ODD = (Z, [(i, (i + 2 * (i % 2) - 1) % 8) for i in range(8)])
ROUTES = {"a": (ODD, FAR, NEAR), "b": (NEAR, EVEN, FAR), "c": (EVEN, NEAR, FAR), "d": (FAR, ODD, NEAR)}


def dot(a, b):
    return jnp.dot(a, b, preferred_element_type=F32)


def picked(array, index):
    return lax.dynamic_index_in_dim(array, index, 0, keepdims=False)


def after(value, *others):
    return lax.optimization_barrier((value, *others))[0]


def moved(value, axis, pairs):
    return lax.ppermute(value, axis, pairs)


def cut(array, widths):
    begin, pieces = 0, []
    for size in widths:
        pieces.append(array[:, begin : begin + size])
        begin += size
    return pieces


def transposed_context(context):
    tokens = context.shape[0]
    core, x, parity = lax.axis_index(C), lax.axis_index(X), lax.axis_index(PARITY)
    rows = context.T.reshape(4, 2, 2, 4, 2, 8, tokens).transpose(4, 3, 1, 0, 2, 5, 6)
    other = moved(picked(rows, 1 - core), C, SWAP)
    rows = jnp.concatenate([picked(rows, core), other], -1).reshape(4, 2, 64, 2 * tokens)

    def block(owner, same):
        return picked(picked(rows, owner), parity if same else 1 - parity)

    at, near, far, across = x, x ^ 1, 3 - x, 3 - (x ^ 1)
    places = {
        "a": tuple([(owner, same) for owner in (at, near, far, across)] for same in (0, 1)),
        "b": ([(near, 1), (across, 1), (near, 0), (across, 0)], [(at, 1), (far, 1), (at, 0), (far, 0)]),
        "c": tuple([(owner, same) for owner in (at, far, near, across)] for same in (0, 1)),
        "d": ([(far, 1), (across, 1), (far, 0), (across, 0)], [(at, 1), (near, 1), (at, 0), (near, 0)]),
    }
    return {
        part: [jnp.concatenate([block(*place) for place in side], 0) for side in sides]
        for part, sides in places.items()
    }


def packed(gain):
    high = lax.reduce_precision(gain, 8, 7)
    return jnp.concatenate([high, gain - high], 0).astype(BF)


def unpacked(rows):
    rows = rows.astype(F32)
    return rows[..., :4, :] + rows[..., 4:, :]


def adam_update(master, first_moment, second_moment, grad_shard):
    new_first = beta_one * first_moment + (1.0 - beta_one) * grad_shard
    new_second = beta_two * second_moment + (1.0 - beta_two) * grad_shard * grad_shard
    new_weight = (master - learn_rate * new_first / (jnp.sqrt(new_second) + adam_floor)).astype(BF)
    return (new_weight, new_first, new_second)


def per_device(context, out_weight, cotangent, norm_gain, first_moment, second_moment):
    tokens, width = cotangent.shape
    ahead, behind = slice(0, AHEAD), slice(AHEAD, tokens)

    def partial(rows, columns):
        own = dot(context[rows], columns).astype(BF)
        return own, moved(own, MP, SWAP)

    first, second = cut(out_weight, FORWARD)
    pieces = [partial(ahead, first), partial(ahead, second), partial(behind, out_weight)]
    context_rows = transposed_context(context)

    def norm_backward(rows, *pieces):
        attn = jnp.concatenate([own.astype(F32) + got.astype(F32) for own, got in pieces], 1)
        inverse = lax.rsqrt(jnp.mean(attn * attn, axis=-1, keepdims=True) + norm_floor)
        normed = attn * inverse
        upstream = cotangent[rows].astype(F32)
        scaled = upstream * norm_gain
        product = jnp.mean(scaled * normed, axis=-1, keepdims=True)
        grads = (inverse * (scaled - normed * product)).astype(BF)
        return grads, jnp.sum(upstream * normed, axis=0)

    context_rows, pieces[1] = lax.optimization_barrier((context_rows, pieces[1]))
    grads_ahead, gain_ahead = norm_backward(ahead, *pieces[:2])
    near_ahead = moved(grads_ahead, C, SWAP)
    near_ahead, pieces[2], gain_ahead = lax.optimization_barrier(
        (near_ahead, pieces[2], gain_ahead)
    )
    grads_behind, gain_behind = norm_backward(behind, pieces[2])
    near_behind = moved(grads_behind, C, SWAP)
    gain = gain_ahead + gain_behind
    near_gain = moved(gain, C, SWAP)

    everyone = (grads_ahead, grads_behind, near_ahead, near_behind)
    whole = [dict(zip(PARTS, cut(part, PARTS.values()))) for part in everyone]
    columns, sent = {}, {}
    for p in PARTS:
        columns[p] = jnp.concatenate([part[p] for part in whole], 0)
        columns[p] = lax.optimization_barrier(columns[p])
        sent[p] = dot(context_rows[p][0], columns[p]).astype(BF)
        if p == "b":
            gain = (gain + after(near_gain, *sent.values())).reshape(4, -1)

    def with_gain(rows):
        spare = ((0, 0), (0, rows.shape[1] - gain.shape[1]))
        return jnp.concatenate([rows, jnp.pad(packed(gain), spare)], 0)

    def product(p, rows):
        return dot(context_rows[p][1][rows], columns[p])

    low, high = slice(0, 128), slice(128, 256)
    sent["c"] = with_gain(sent["c"])
    first = {p: moved(rows, *ROUTES[p][0]) for p, rows in sent.items()}
    second, kept = {}, {}
    for p in PARTS:
        rows = (product(p, high) + first[p][high].astype(F32)).astype(BF)
        if p == "c":
            gain += unpacked(after(first["c"][256:], rows))
        second[p] = moved(with_gain(rows) if p == "c" else rows, *ROUTES[p][1])
    for p in PARTS:
        kept[p] = product(p, low) + first[p][low].astype(F32)
    gain += unpacked(second["c"][128:])

    def joined(one, other, wrap):
        parts = (one, other)
        rows = [kept[p][64:] + second[p][64:128].astype(F32) for p in parts]
        rows = wrap(jnp.concatenate(rows, 1).astype(BF))
        got = moved(rows, *ROUTES[one][2])
        rows = [kept[p][:64] + second[p][:64].astype(F32) for p in parts]
        return jnp.concatenate(rows, 1) + got[:64].astype(F32), got[64:]

    left, gains = joined("b", "c", with_gain)
    right, _ = joined("a", "d", lambda rows: rows)
    gain += unpacked(gains[:, : gain.shape[1]])
    left, right, gains = lax.optimization_barrier(
        (left.astype(BF), right.astype(BF), packed(gain))
    )
    tiles = jnp.concatenate(
        [
            left.reshape(8, 8, -1),
            right.reshape(8, 8, -1),
            jnp.broadcast_to(gains, (8, *gains.shape)),
        ],
        -1,
    )
    arrived = lax.all_to_all(tiles, (QUAD, YL), split_axis=0, concat_axis=0, tiled=True)
    grads = [after(part, tiles) for part in (grads_ahead, grads_behind)]
    grad_context = lax.dot_general(
        jnp.concatenate(grads, 0),
        out_weight,
        (((1,), (1,)), ((), ())),
        preferred_element_type=F32,
    ).astype(BF)
    tiles, grad_context = lax.optimization_barrier((arrived, grad_context))
    grad_gain = unpacked(tiles[..., width:]).sum(0).reshape(-1)
    grad_shard = tiles[..., :width].astype(F32).sum(0)
    part_b, part_c, part_a, part_d = cut(grad_shard, [PARTS[p] for p in "bcad"])
    grad_shard = jnp.concatenate([part_a, part_b, part_c, part_d], 1)

    shard_rows = first_moment.shape[1]
    master = lax.dynamic_slice_in_dim(
        out_weight, lax.axis_index(DP) * shard_rows, shard_rows, 0
    ).astype(F32)[None]
    new_weight, new_first, new_second = adam_update(
        master, first_moment, second_moment, grad_shard[None]
    )
    return (new_weight, new_first, new_second, grad_gain, grad_context)


def solution(mesh):
    finer = Mesh(mesh.devices.reshape(4, 2, 2, 4, 2, mesh.shape["mp"]), (*DP, MP))
    placed = (P(DP, MP), P(MP, None), P(DP, None), P(), P(MP, DP, None), P(MP, DP, None))
    return jax.shard_map(
        per_device,
        mesh=finer,
        in_specs=placed,
        out_specs=(P(MP, DP, None), P(MP, DP, None), P(MP, DP, None), P(), P(DP, MP)),
        check_vma=False,
    )
```
